32 devices in a mesh: row: 8 (over y, x, core), col: 4 (over z).
Axes of the slice: x: 2, y: 2, z: 4, core: 2. Of those that a mesh axis runs over, the one named last changes fastest.
Arguments:
- features: bfloat16 [16384, 256], P(('row', 'col')), may hold values from -1 to 3
- in_degree: int32 [16384], P(('row', 'col')), may hold values from 512 to 2047
- tile_index: int32 [8192, 2], P(('row', 'col')), may hold values from 0 to 31, as said below
- tile_count: int32 [32], P(('row', 'col')), may hold values from 1 to 256, as said below
- adjacency_tiles: bfloat16 [8192, 128, 128], P(('row', 'col')), may hold values from 0 to 1, as said below
- projection: bfloat16 [512, 256], replicated, may hold values from -0.25 to 0.25
- out_bias: float32 [256], replicated, may hold values from -3 to 3
Outputs:
- hidden_out: bfloat16 [16384, 256], P(('row', 'col'))
The draws below stay inside these ranges and needn't reach their ends.
Inputs may be any that keep to these rules, and one draw needn't show every extreme that they name: `tile_index`: column 0 is a local row block below 16, column 1 a local column block below 32, in every slot. `tile_count`: slots at or beyond the count hold tiles and indices that must be ignored; some device has all 256 slots live in every draw. `adjacency_tiles`: entries are 0 or 1.
All inputs are finite; a program needn't handle non-finite values.
Results may differ from the reference program's by a relative error of at most 0.0034.
Values may be sent and summed in bfloat16 or wider, within the bound.
A program may use at most 128 MiB of HBM per device.

```python
import jax
import jax.numpy as jnp
from jax import lax

F = 256
H = 256
TILE = 128
VB_DEV = 4
MAX_TILES = 256
RB = 16
CB = 32
V = 16384
N_ROW = 8
N_COL = 4


def draw_tile_index(key, part):
    slots = N_ROW * N_COL * MAX_TILES
    row_part = jax.random.randint(jax.random.fold_in(key, 11), (slots,), 0, VB_DEV * N_COL)
    col_part = jax.random.randint(jax.random.fold_in(key, 12), (slots,), 0, VB_DEV * N_ROW)
    return jnp.stack([row_part, col_part], axis=1).astype(jnp.int32)


def draw_tile_count(key, part):
    devices = N_ROW * N_COL
    counts = jax.random.randint(jax.random.fold_in(key, 21), (devices,), max(1, MAX_TILES // 8), MAX_TILES + 1)
    fullest = jax.random.randint(jax.random.fold_in(key, 22), (), 0, devices)
    placed = jnp.arange(devices, dtype=jnp.int32) == fullest
    return jnp.where(placed, MAX_TILES, counts).astype(jnp.int32)


def draw_adjacency_tiles(key, part):
    shape = (N_ROW * N_COL * MAX_TILES, TILE, TILE)
    uniform_draw = jax.random.uniform(jax.random.fold_in(key, 31), shape, jnp.float32)
    return jnp.where(uniform_draw < 0.25, 1.0, 0.0).astype(jnp.float32).astype(jnp.bfloat16)


def place_ends(drawn, own_key, low, largest):
    longest = drawn.shape.index(max(drawn.shape))
    spots = []
    for shift in (0, 1):
        where = [jax.random.randint(jax.random.fold_in(own_key, axis), (), 0, length) for axis, length in enumerate(drawn.shape)]
        where[longest] = (where[longest] + shift) % drawn.shape[longest]
        spots.append(tuple(where))
    return drawn.at[spots[0]].set(low).at[spots[1]].set(largest)


def shard_levels(own_key, extent, split, low, largest):
    def one(axis_at, parts):
        heights = jax.random.uniform(jax.random.fold_in(jax.random.fold_in(own_key, 6), axis_at), (parts,), jnp.float32, low / len(split), largest / len(split))
        return jnp.repeat(jnp.exp(heights), extent[axis_at] // parts).reshape((-1,) + (1,) * (len(extent) - axis_at - 1))

    level = one(*split[0])
    for cut in split[1:]:
        level = level * one(*cut)
    return level


def centred(key, dims, width, limit, held_as=jnp.bfloat16):
    array = jax.random.normal(key, dims, jnp.float32) * width
    return jnp.minimum(jnp.maximum(array, -limit), limit).astype(held_as)


def setup_inputs(seed: int = 0) -> dict:
    keys = jax.random.split(jax.random.key(seed), 8)
    features = jnp.clip(-1.0 + 4.0 * jax.random.uniform(keys[0], (V, F), jnp.float32) ** shard_levels(keys[0], (V, F), ((0, 32),), -0.2, 0.2), -1.0, 3.0).astype(jnp.bfloat16)
    in_degree = place_ends(jax.random.randint(keys[1], (V,), max(1, MAX_TILES * TILE // (VB_DEV * 16)), max(2, MAX_TILES * TILE // (VB_DEV * 4))), jax.random.fold_in(keys[1], 1), max(1, MAX_TILES * TILE // (VB_DEV * 16)), (max(2, MAX_TILES * TILE // (VB_DEV * 4))) - 1).astype(jnp.int32)
    tile_index = draw_tile_index(jax.random.fold_in(keys[7], 71), 0)
    tile_count = draw_tile_count(jax.random.fold_in(keys[7], 71), 0)
    adjacency_tiles = draw_adjacency_tiles(jax.random.fold_in(keys[7], 71), 0)
    projection = centred(keys[5], (2 * F, H), (2 * F) ** -0.5, 0.25)
    out_bias = centred(keys[6], (H,), 0.5, 3.0, jnp.float32)
    return {"features": features, "in_degree": in_degree, "tile_index": tile_index, "tile_count": tile_count, "adjacency_tiles": adjacency_tiles, "projection": projection, "out_bias": out_bias}


def device_partial(column_rows, slot_index, live_count, slot_tiles):
    blocks = column_rows.reshape(CB, TILE, F).astype(jnp.float32)[slot_index[:, 1]]
    alive = (jnp.arange(MAX_TILES, dtype=jnp.int32) < live_count).astype(jnp.float32)
    masked = slot_tiles.astype(jnp.float32) * alive[:, None, None]
    product = jnp.einsum("kij,kjf->kif", masked, blocks)
    summed = jax.ops.segment_sum(product, slot_index[:, 0], num_segments=RB)
    return summed.reshape(RB * TILE, F)


def reference(features, in_degree, tile_index, tile_count, adjacency_tiles, projection, out_bias):
    span = VB_DEV * TILE
    grouped = features.reshape(N_ROW, N_COL, span, F)

    def per_row(row_id):
        def per_col(running, col_id):
            column_rows = jnp.take(grouped, col_id, axis=1).reshape(N_ROW * span, F)
            device = row_id * N_COL + col_id
            slot_index = lax.dynamic_slice_in_dim(tile_index, device * MAX_TILES, MAX_TILES, 0)
            slot_tiles = lax.dynamic_slice_in_dim(adjacency_tiles, device * MAX_TILES, MAX_TILES, 0)
            live_count = tile_count[device]
            return running + device_partial(column_rows, slot_index, live_count, slot_tiles), None

        zeroed = jnp.zeros((RB * TILE, F), jnp.float32)
        summed, _ = lax.scan(per_col, zeroed, jnp.arange(N_COL, dtype=jnp.int32))
        return summed

    sums = lax.map(per_row, jnp.arange(N_ROW, dtype=jnp.int32)).reshape(V, F)
    neighbour_mean = (sums / in_degree[:, None].astype(jnp.float32)).astype(jnp.bfloat16)
    joined = jnp.concatenate([features, neighbour_mean], axis=1)
    mixed = jnp.dot(joined, projection, preferred_element_type=jnp.float32) + out_bias[None, :]
    return jnp.maximum(mixed, 0.0).astype(jnp.bfloat16)
```

```python
import functools

import jax
import jax.numpy as jnp
from jax import lax
from jax.experimental import pallas as pl
from jax.experimental.pallas import tpu as pltpu
from jax.sharding import PartitionSpec as P

BLK = 32
LANES = 128
CHUNKS = 16
DENSE_LIMIT = 24 * 1024 * 1024
MESH = pl.DeviceIdType.MESH


def block_terms(running, col_blocks, index_block, tile_block, live_block):
    picked = col_blocks[index_block[:, 1]]
    kept = jnp.where(live_block[:, None, None], tile_block, jnp.zeros_like(tile_block))
    product = jnp.einsum("kij,kjf->kif", kept, picked, preferred_element_type=jnp.float32)
    flattened = product.reshape(product.shape[0], -1)
    return running.at[index_block[:, 0]].add(flattened)


def local_sparse(features, in_degree, tile_index, tile_count, adjacency_tiles, projection, out_bias):
    feat_width = features.shape[1]
    tile_size = adjacency_tiles.shape[1]
    slot_total = adjacency_tiles.shape[0]
    gathered = lax.all_gather(features, "row", axis=0, tiled=True)
    col_blocks = gathered.reshape(gathered.shape[0] // tile_size, tile_size, feat_width)
    row_blocks = features.shape[0] * lax.axis_size("col") // tile_size
    live_count = tile_count[0]
    zeroed = jnp.zeros((row_blocks, tile_size * feat_width), jnp.float32)

    def one_step(running, offset):
        index_block = lax.dynamic_slice_in_dim(tile_index, offset, BLK, 0)
        tile_block = lax.dynamic_slice_in_dim(adjacency_tiles, offset, BLK, 0)
        live_block = offset + jnp.arange(BLK, dtype=jnp.int32) < live_count
        return (block_terms(running, col_blocks, index_block, tile_block, live_block), None)

    summed, _ = lax.scan(one_step, zeroed, jnp.arange(0, slot_total, BLK, dtype=jnp.int32))
    partial_value = summed.reshape(row_blocks * tile_size, feat_width)
    own_sums = lax.psum_scatter(partial_value, "col", scatter_dimension=0, tiled=True)
    neighbour_mean = (own_sums / in_degree[:, None].astype(jnp.float32)).astype(jnp.bfloat16)
    joined = jnp.concatenate([features, neighbour_mean], axis=1)
    mixed = jnp.dot(joined, projection, preferred_element_type=jnp.float32) + out_bias[None, :]
    return jnp.maximum(mixed, 0.0).astype(jnp.bfloat16)


def densify_kernel(row_blocks, count_ref, place_ref, tiles_ref, dense_ref, stage, sems):
    slots, tile = stage.shape[0], stage.shape[1]
    per = slots // CHUNKS

    def load(i):
        part = pl.ds(i * per, per)
        return pltpu.make_async_copy(tiles_ref.at[part], stage.at[part], sems.at[i])

    for i in range(CHUNKS):
        load(i).start()

    @pl.loop(0, dense_ref.shape[0])
    def _(j):
        dense_ref[j] = jnp.zeros(dense_ref.shape[1:], dense_ref.dtype)

    count = count_ref[0]
    for i in range(CHUNKS):
        load(i).wait()

        @pl.loop(i * per, jnp.minimum((i + 1) * per, jnp.maximum(count, i * per)))
        def _(slot):
            place = place_ref[slot]
            col = place // row_blocks
            row = pl.multiple_of((place - col * row_blocks) * tile, tile)
            dense_ref[col, pl.ds(row, tile), :] += stage[slot]


def fused_kernel(n_row, n_col, feat_ref, dense_ref, degree_ref, proj_ref, bias_ref, out_ref,
                 gathered, acc, hidden, degree_col, send_r, recv_r, send_l, recv_l,
                 ag_send, ag_recv, sr_sem, rr_sem, sl_sem, rl_sem):
    seg, width = feat_ref.shape
    halves = width // LANES
    blocks = seg // LANES
    chips = n_row // 2
    r = lax.axis_index("row")
    c = lax.axis_index("col")
    sibling = r ^ 1

    barrier = pltpu.get_barrier_semaphore()

    def greet(row, col):
        pl.semaphore_signal(barrier, inc=1, device_id=(row, col), device_id_type=MESH)

    greet(sibling, c)
    for m in range(1, chips):
        greet(r ^ (2 * m), c)

    @pl.when(c > 0)
    def _():
        greet(r, c - 1)

    @pl.when(c < n_col - 1)
    def _():
        greet(r, c + 1)

    pl.semaphore_wait(
        barrier, chips + jnp.where(c > 0, 1, 0) + jnp.where(c < n_col - 1, 1, 0))

    def lanes(h):
        return pl.ds(h * LANES, LANES)

    def gather_copy(h, j):
        if j == 0:
            src, owner, target = feat_ref.at[:, lanes(h)], r, sibling
        elif j < chips:
            src, owner, target = feat_ref.at[:, lanes(h)], r, r ^ (2 * j)
        else:
            owner = r ^ (2 * (j - chips + 1))
            src, target = gathered.at[owner, :, lanes(h)], sibling
        return pltpu.make_async_remote_copy(
            src_ref=src, dst_ref=gathered.at[owner, :, lanes(h)],
            send_sem=ag_send.at[h, j], recv_sem=ag_recv.at[h, j],
            device_id=(target, c), device_id_type=MESH)

    def source(j):
        if j == 0:
            return sibling
        if j < chips:
            return r ^ (2 * j)
        return sibling ^ (2 * (j - chips + 1))

    total = 2 * chips - 1
    for h in range(halves):
        for j in range(1, chips):
            gather_copy(h, j).start()
        gather_copy(h, 0).start()

    def multiply(h, owner, block, first):
        @pl.loop(0, n_col)
        def _(d):
            rows = pl.ds(pl.multiple_of(d * seg, seg), seg)
            left = jnp.concatenate(
                [dense_ref[owner * blocks + k, rows, :] for k in range(blocks)], axis=1)
            product = jnp.dot(left, block, preferred_element_type=jnp.float32)
            if first:
                acc[h, rows, :] = product
            else:
                acc[h, rows, :] += product

    def own_block(h):
        multiply(h, r, feat_ref[:, lanes(h)], True)

    def other_block(h, j):
        gather_copy(h, j).wait_recv()
        if 0 < j < chips:
            gather_copy(h, j + chips - 1).start()
        owner = source(j)
        multiply(h, owner, gathered[owner, :, lanes(h)], False)

    def right_copy(h, d):
        return pltpu.make_async_remote_copy(
            src_ref=send_r.at[h, d], dst_ref=recv_r.at[h, d],
            send_sem=sr_sem.at[h, d], recv_sem=rr_sem.at[h, d],
            device_id=(r, c + 1), device_id_type=MESH)

    def left_copy(h, d):
        return pltpu.make_async_remote_copy(
            src_ref=send_l.at[h, d], dst_ref=recv_l.at[h, d],
            send_sem=sl_sem.at[h, d], recv_sem=rl_sem.at[h, d],
            device_id=(r, c - 1), device_id_type=MESH)

    def term(h, d):
        return acc[h, d * seg:(d + 1) * seg, :]

    def begin(h):
        @pl.when(c == 0)
        def _():
            for d in range(n_col - 1, 0, -1):
                send_r[h, d] = term(h, d).astype(send_r.dtype)
                right_copy(h, d).start()

        @pl.when(c == n_col - 1)
        def _():
            for d in range(n_col - 1):
                send_l[h, d] = term(h, d).astype(send_l.dtype)
                left_copy(h, d).start()

    def relay(h, t):
        d = n_col - 1 - t

        @pl.when((c > 0) & (c < d))
        def _():
            right_copy(h, d).wait_recv()
            send_r[h, d] = (term(h, d) + recv_r[h, d].astype(jnp.float32)).astype(send_r.dtype)
            right_copy(h, d).start()

        @pl.when((c < n_col - 1) & (c > t))
        def _():
            left_copy(h, t).wait_recv()
            send_l[h, t] = (term(h, t) + recv_l[h, t].astype(jnp.float32)).astype(send_l.dtype)
            left_copy(h, t).start()

    def finish(h):
        own = pl.ds(pl.multiple_of(c * seg, seg), seg)

        @pl.when(c > 0)
        def _():
            right_copy(h, c).wait_recv()
            acc[h, own, :] += recv_r[h, c].astype(jnp.float32)

        @pl.when(c < n_col - 1)
        def _():
            left_copy(h, c).wait_recv()
            acc[h, own, :] += recv_l[h, c].astype(jnp.float32)

        mean = (acc[h, own, :] / degree_col[...]).astype(jnp.bfloat16)
        hidden[...] += jnp.dot(
            mean, proj_ref[width + h * LANES:width + (h + 1) * LANES, :],
            preferred_element_type=jnp.float32)

    for h in range(halves):
        own_block(h)
        if h == 0:
            hidden[...] = jnp.dot(
                feat_ref[...], proj_ref[:width, :],
                preferred_element_type=jnp.float32) + bias_ref[...]
            for b in range(blocks):
                one = degree_ref[b:b + 1, :].astype(jnp.float32)
                degree_col[b * LANES:(b + 1) * LANES, :] = jnp.transpose(
                    jnp.broadcast_to(one, (LANES, LANES)))
        for j in range(total):
            other_block(h, j)
            if h > 0 and j >= 2 and j % 2 == 0 and (j - 2) // 2 < n_col - 2:
                relay(h - 1, (j - 2) // 2)
        begin(h)
        if h > 0:
            finish(h - 1)
    for t in range(n_col - 2):
        relay(halves - 1, t)
    finish(halves - 1)
    out_ref[...] = jnp.maximum(hidden[...], 0.0).astype(out_ref.dtype)

    for h in range(halves):
        for j in range(total):
            gather_copy(h, j).wait_send()
        for d in range(n_col):
            if d > 0:
                @pl.when(c < d)
                def _():
                    right_copy(h, d).wait_send()
            if d < n_col - 1:
                @pl.when(c > d)
                def _():
                    left_copy(h, d).wait_send()


def local_dense(n_row, n_col, features, in_degree, tile_index, tile_count, adjacency_tiles, projection, out_bias):
    seg, width = features.shape
    slots, tile, _ = adjacency_tiles.shape
    row_blocks = seg * n_col // tile
    col_blocks = seg * n_row // tile
    halves = width // LANES
    vmem = pl.BlockSpec(memory_space=pltpu.VMEM)
    smem = pl.BlockSpec(memory_space=pltpu.SMEM)
    place = tile_index[:, 0] + tile_index[:, 1] * row_blocks
    dense = pl.pallas_call(
        functools.partial(densify_kernel, row_blocks),
        out_shape=pltpu.VMEM((col_blocks, row_blocks * tile, tile), jnp.bfloat16),
        in_specs=[smem, smem, pl.BlockSpec(memory_space=pl.ANY)],
        out_specs=vmem,
        scratch_shapes=[
            pltpu.VMEM((slots, tile, tile), jnp.bfloat16),
            pltpu.SemaphoreType.DMA((CHUNKS,)),
        ],
        compiler_params=pltpu.CompilerParams(vmem_limit_bytes=42 * 1024 * 1024),
    )(tile_count, place, adjacency_tiles)
    carry = pltpu.VMEM((halves, n_col, seg, LANES), jnp.bfloat16)
    carry_sem = pltpu.SemaphoreType.DMA((halves, n_col))
    gather_sem = pltpu.SemaphoreType.DMA((halves, n_row))
    return pl.pallas_call(
        functools.partial(fused_kernel, n_row, n_col),
        out_shape=jax.ShapeDtypeStruct((seg, projection.shape[1]), jnp.bfloat16),
        in_specs=[vmem] * 5,
        out_specs=vmem,
        scratch_shapes=[
            pltpu.VMEM((n_row, seg, width), jnp.bfloat16),
            pltpu.VMEM((halves, n_col * seg, LANES), jnp.float32),
            pltpu.VMEM((seg, projection.shape[1]), jnp.float32),
            pltpu.VMEM((seg, LANES), jnp.float32),
            carry, carry, carry, carry,
            gather_sem, gather_sem,
            carry_sem, carry_sem, carry_sem, carry_sem,
        ],
        compiler_params=pltpu.CompilerParams(
            collective_id=0, has_side_effects=True, vmem_limit_bytes=24 * 1024 * 1024),
    )(features, dense, in_degree.reshape(seg // LANES, LANES), projection, out_bias[None, :])


def solution(mesh):
    n_row, n_col = mesh.shape["row"], mesh.shape["col"]

    def local(features, in_degree, tile_index, tile_count, adjacency_tiles, projection, out_bias):
        seg, width = features.shape
        slots, tile, _ = adjacency_tiles.shape
        dense_bytes = 2 * seg * n_row * seg * n_col
        fits = (
            dense_bytes <= DENSE_LIMIT and slots <= 256 and slots % CHUNKS == 0
            and tile == LANES and seg % LANES == 0 and width % LANES == 0
            and n_row >= 4 and n_row & (n_row - 1) == 0 and n_col >= 2)
        args = (features, in_degree, tile_index, tile_count, adjacency_tiles, projection, out_bias)
        return local_dense(n_row, n_col, *args) if fits else local_sparse(*args)

    return jax.shard_map(
        local,
        mesh=mesh,
        in_specs=(
            P(("row", "col"), None),
            P(("row", "col")),
            P(("row", "col"), None),
            P(("row", "col")),
            P(("row", "col"), None, None),
            P(),
            P(),
        ),
        out_specs=P(("row", "col"), None),
        check_vma=False,
    )
```

```python
import functools

import jax
import jax.numpy as jnp
from jax import lax
from jax.experimental import pallas as pl
from jax.experimental.pallas import tpu as pltpu
from jax.sharding import PartitionSpec as P

BLK = 32
LANES = 128
CHUNKS = 16
DENSE_LIMIT = 24 * 1024 * 1024
MESH = pl.DeviceIdType.MESH


def block_terms(running, col_blocks, index_block, tile_block, live_block):
    picked = col_blocks[index_block[:, 1]]
    kept = jnp.where(live_block[:, None, None], tile_block, jnp.zeros_like(tile_block))
    product = jnp.einsum("kij,kjf->kif", kept, picked, preferred_element_type=jnp.float32)
    flattened = product.reshape(product.shape[0], -1)
    return running.at[index_block[:, 0]].add(flattened)


def local_sparse(features, in_degree, tile_index, tile_count, adjacency_tiles, projection, out_bias):
    feat_width = features.shape[1]
    tile_size = adjacency_tiles.shape[1]
    slot_total = adjacency_tiles.shape[0]
    gathered = lax.all_gather(features, "row", axis=0, tiled=True)
    col_blocks = gathered.reshape(gathered.shape[0] // tile_size, tile_size, feat_width)
    row_blocks = features.shape[0] * lax.axis_size("col") // tile_size
    live_count = tile_count[0]
    zeroed = jnp.zeros((row_blocks, tile_size * feat_width), jnp.float32)

    def one_step(running, offset):
        index_block = lax.dynamic_slice_in_dim(tile_index, offset, BLK, 0)
        tile_block = lax.dynamic_slice_in_dim(adjacency_tiles, offset, BLK, 0)
        live_block = offset + jnp.arange(BLK, dtype=jnp.int32) < live_count
        return (block_terms(running, col_blocks, index_block, tile_block, live_block), None)

    summed, _ = lax.scan(one_step, zeroed, jnp.arange(0, slot_total, BLK, dtype=jnp.int32))
    partial_value = summed.reshape(row_blocks * tile_size, feat_width)
    own_sums = lax.psum_scatter(partial_value, "col", scatter_dimension=0, tiled=True)
    neighbour_mean = (own_sums / in_degree[:, None].astype(jnp.float32)).astype(jnp.bfloat16)
    joined = jnp.concatenate([features, neighbour_mean], axis=1)
    mixed = jnp.dot(joined, projection, preferred_element_type=jnp.float32) + out_bias[None, :]
    return jnp.maximum(mixed, 0.0).astype(jnp.bfloat16)


def densify_kernel(row_blocks, count_ref, place_ref, tiles_ref, dense_ref, stage, sems):
    slots, tile = stage.shape[0], stage.shape[1]
    per = slots // CHUNKS

    def load(i):
        part = pl.ds(i * per, per)
        return pltpu.make_async_copy(tiles_ref.at[part], stage.at[part], sems.at[i])

    for i in range(CHUNKS):
        load(i).start()

    @pl.loop(0, dense_ref.shape[0])
    def _(j):
        dense_ref[j] = jnp.zeros(dense_ref.shape[1:], dense_ref.dtype)

    count = count_ref[0]
    for i in range(CHUNKS):
        load(i).wait()

        @pl.loop(i * per, jnp.minimum((i + 1) * per, jnp.maximum(count, i * per)))
        def _(slot):
            place = place_ref[slot]
            col = place // row_blocks
            row = pl.multiple_of((place - col * row_blocks) * tile, tile)
            dense_ref[col, pl.ds(row, tile), :] += stage[slot]


def fused_kernel(n_row, n_col, feat_ref, dense_ref, degree_ref, proj_ref, bias_ref, out_ref,
                 gathered, acc, hidden, degree_col, send, relayed, landed,
                 ag_send, ag_recv, send_sem, relay_sem, land_sem):
    seg, width = feat_ref.shape
    halves = width // LANES
    blocks = seg // LANES
    chips = n_row // 2
    r = lax.axis_index("row")
    c = lax.axis_index("col")
    sibling = r ^ 1

    barrier = pltpu.get_barrier_semaphore()

    def greet(row, col):
        pl.semaphore_signal(barrier, inc=1, device_id=(row, col), device_id_type=MESH)

    greet(sibling, c)
    for m in range(1, chips):
        greet(r ^ (2 * m), c)

    peers = chips
    for hop in range(1, n_col):
        for step in (-hop, hop):
            inside = (c + step >= 0) & (c + step < n_col)
            peers = peers + jnp.where(inside, 1, 0)

            @pl.when(inside)
            def _():
                greet(r, c + step)

    pl.semaphore_wait(barrier, peers)

    def lanes(h):
        return pl.ds(h * LANES, LANES)

    def gather_copy(h, j):
        if j == 0:
            src, owner, target = feat_ref.at[:, lanes(h)], r, sibling
        elif j < chips:
            src, owner, target = feat_ref.at[:, lanes(h)], r, r ^ (2 * j)
        else:
            owner = r ^ (2 * (j - chips + 1))
            src, target = gathered.at[owner, :, lanes(h)], sibling
        return pltpu.make_async_remote_copy(
            src_ref=src, dst_ref=gathered.at[owner, :, lanes(h)],
            send_sem=ag_send.at[h, j], recv_sem=ag_recv.at[h, j],
            device_id=(target, c), device_id_type=MESH)

    def source(j):
        if j == 0:
            return sibling
        if j < chips:
            return r ^ (2 * j)
        return sibling ^ (2 * (j - chips + 1))

    total = 2 * chips - 1

    def gather_start(h):
        for j in range(1, chips):
            gather_copy(h, j).start()
        gather_copy(h, 0).start()

    gather_start(0)

    def multiply(h, owner, block, first):
        @pl.loop(0, n_col)
        def _(d):
            rows = pl.ds(pl.multiple_of(d * seg, seg), seg)
            left = jnp.concatenate(
                [dense_ref[owner * blocks + k, rows, :] for k in range(blocks)], axis=1)
            product = jnp.dot(left, block, preferred_element_type=jnp.float32)
            if first:
                acc[h, rows, :] = product
            else:
                acc[h, rows, :] += product

    def own_block(h):
        multiply(h, r, feat_ref[:, lanes(h)], True)

    def other_block(h, j):
        gather_copy(h, j).wait_recv()
        if 0 < j < chips:
            gather_copy(h, j + chips - 1).start()
        owner = source(j)
        multiply(h, owner, gathered[owner, :, lanes(h)], False)

    def term(h, d):
        return acc[h, d * seg:(d + 1) * seg, :]

    def relay_copy(h, d, way):
        return pltpu.make_async_remote_copy(
            src_ref=send.at[h, d], dst_ref=relayed.at[h],
            send_sem=send_sem.at[h, d], recv_sem=relay_sem.at[h],
            device_id=(r, c + way), device_id_type=MESH)

    def land_copy(h, d, slot):
        return pltpu.make_async_remote_copy(
            src_ref=send.at[h, d], dst_ref=landed.at[h, slot],
            send_sem=send_sem.at[h, d], recv_sem=land_sem.at[h, slot],
            device_id=(r, d), device_id_type=MESH)

    def routes():
        for d in range(n_col - 1, -1, -1):
            for c_from in range(n_col):
                if c_from != d:
                    yield d, c_from, abs(d - c_from), 1 if d > c_from else -1

    def slot_of(hops, way):
        return hops - 1 + (0 if way > 0 else 2)

    def adds_relay(d, c_from, hops, way):
        return hops == 2 and 0 <= c_from - way < n_col

    def relays(c_from):
        return n_col == 4 and c_from in (0, n_col - 1)

    def send_direct(h, d, hops, way):
        send[h, d] = term(h, d).astype(send.dtype)
        land_copy(h, d, slot_of(hops, way)).start()

    def first_sends(h):
        for d, c_from, hops, way in routes():
            if hops == 3:
                @pl.when(c == c_from)
                def _():
                    send[h, d] = term(h, d).astype(send.dtype)
                    relay_copy(h, d, way).start()
            elif not relays(c_from) and not adds_relay(d, c_from, hops, way):
                @pl.when(c == c_from)
                def _():
                    send_direct(h, d, hops, way)

    def later_sends(h):
        for c_from in range(n_col):
            if relays(c_from):
                @pl.when(c == c_from)
                def _():
                    far = n_col - 1 - c_from
                    way = 1 if far > c_from else -1
                    relay_copy(h, far, way).wait_send()
                    for hops in (2, 1):
                        send_direct(h, c_from + way * hops, hops, way)

    def relay_sends(h):
        for d, c_from, hops, way in routes():
            if adds_relay(d, c_from, hops, way):
                @pl.when(c == c_from)
                def _():
                    relay_copy(h, d, way).wait_recv()
                    send[h, d] = (term(h, d) + relayed[h].astype(jnp.float32)).astype(send.dtype)
                    land_copy(h, d, slot_of(hops, way)).start()

    def finish(h):
        own = pl.ds(pl.multiple_of(c * seg, seg), seg)
        for hops in (1, 2):
            for way in (1, -1):
                origin = c - way * hops

                @pl.when((origin >= 0) & (origin < n_col))
                def _():
                    slot = slot_of(hops, way)
                    land_copy(h, 0, slot).wait_recv()
                    acc[h, own, :] += landed[h, slot].astype(jnp.float32)

        mean = (acc[h, own, :] / degree_col[...]).astype(jnp.bfloat16)
        hidden[...] += jnp.dot(
            mean, proj_ref[width + h * LANES:width + (h + 1) * LANES, :],
            preferred_element_type=jnp.float32)

    for h in range(halves):
        own_block(h)
        if h == 0:
            hidden[...] = jnp.dot(
                feat_ref[...], proj_ref[:width, :],
                preferred_element_type=jnp.float32) + bias_ref[...]
            for b in range(blocks):
                one = degree_ref[b:b + 1, :].astype(jnp.float32)
                degree_col[b * LANES:(b + 1) * LANES, :] = jnp.transpose(
                    jnp.broadcast_to(one, (LANES, LANES)))
        for j in range(total):
            if h > 0 and j == 1:
                later_sends(h - 1)
                relay_sends(h - 1)
            other_block(h, j)
            if j == chips - 1 and h + 1 < halves:
                gather_start(h + 1)
        first_sends(h)
        if h > 0:
            finish(h - 1)
    later_sends(halves - 1)
    relay_sends(halves - 1)
    finish(halves - 1)
    out_ref[...] = jnp.maximum(hidden[...], 0.0).astype(out_ref.dtype)

    for h in range(halves):
        for j in range(total):
            gather_copy(h, j).wait_send()
        for d, c_from, hops, way in routes():
            if hops < 3:
                @pl.when(c == c_from)
                def _():
                    land_copy(h, d, slot_of(hops, way)).wait_send()


def local_dense(n_row, n_col, features, in_degree, tile_index, tile_count, adjacency_tiles, projection, out_bias):
    seg, width = features.shape
    slots, tile, _ = adjacency_tiles.shape
    row_blocks = seg * n_col // tile
    col_blocks = seg * n_row // tile
    halves = width // LANES
    vmem = pl.BlockSpec(memory_space=pltpu.VMEM)
    smem = pl.BlockSpec(memory_space=pltpu.SMEM)
    place = tile_index[:, 0] + tile_index[:, 1] * row_blocks
    dense = pl.pallas_call(
        functools.partial(densify_kernel, row_blocks),
        out_shape=pltpu.VMEM((col_blocks, row_blocks * tile, tile), jnp.bfloat16),
        in_specs=[smem, smem, pl.BlockSpec(memory_space=pl.ANY)],
        out_specs=vmem,
        scratch_shapes=[
            pltpu.VMEM((slots, tile, tile), jnp.bfloat16),
            pltpu.SemaphoreType.DMA((CHUNKS,)),
        ],
        compiler_params=pltpu.CompilerParams(vmem_limit_bytes=42 * 1024 * 1024),
    )(tile_count, place, adjacency_tiles)
    carry_sem = pltpu.SemaphoreType.DMA((halves, 4))
    gather_sem = pltpu.SemaphoreType.DMA((halves, n_row))
    return pl.pallas_call(
        functools.partial(fused_kernel, n_row, n_col),
        out_shape=jax.ShapeDtypeStruct((seg, projection.shape[1]), jnp.bfloat16),
        in_specs=[vmem] * 5,
        out_specs=vmem,
        scratch_shapes=[
            pltpu.VMEM((n_row, seg, width), jnp.bfloat16),
            pltpu.VMEM((halves, n_col * seg, LANES), jnp.float32),
            pltpu.VMEM((seg, projection.shape[1]), jnp.float32),
            pltpu.VMEM((seg, LANES), jnp.float32),
            pltpu.VMEM((halves, n_col, seg, LANES), jnp.bfloat16),
            pltpu.VMEM((halves, seg, LANES), jnp.bfloat16),
            pltpu.VMEM((halves, 4, seg, LANES), jnp.bfloat16),
            gather_sem, gather_sem,
            carry_sem, pltpu.SemaphoreType.DMA((halves,)), carry_sem,
        ],
        compiler_params=pltpu.CompilerParams(
            collective_id=0, has_side_effects=True, vmem_limit_bytes=24 * 1024 * 1024),
    )(features, dense, in_degree.reshape(seg // LANES, LANES), projection, out_bias[None, :])


def solution(mesh):
    n_row, n_col = mesh.shape["row"], mesh.shape["col"]

    def local(features, in_degree, tile_index, tile_count, adjacency_tiles, projection, out_bias):
        seg, width = features.shape
        slots, tile, _ = adjacency_tiles.shape
        dense_bytes = 2 * seg * n_row * seg * n_col
        fits = (
            dense_bytes <= DENSE_LIMIT and slots <= 256 and slots % CHUNKS == 0
            and tile == LANES and seg % LANES == 0 and width % LANES == 0
            and n_row >= 4 and n_row & (n_row - 1) == 0 and 2 <= n_col <= 4)
        args = (features, in_degree, tile_index, tile_count, adjacency_tiles, projection, out_bias)
        return local_dense(n_row, n_col, *args) if fits else local_sparse(*args)

    return jax.shard_map(
        local,
        mesh=mesh,
        in_specs=(
            P(("row", "col"), None),
            P(("row", "col")),
            P(("row", "col"), None),
            P(("row", "col")),
            P(("row", "col"), None, None),
            P(),
            P(),
        ),
        out_specs=P(("row", "col"), None),
        check_vma=False,
    )
```

```python
import functools

import jax
import jax.numpy as jnp
from jax import lax
from jax.experimental import pallas as pl
from jax.experimental.pallas import tpu as pltpu
from jax.sharding import PartitionSpec as P

BLK = 32
LANES = 128
CHUNKS = 16
DENSE_LIMIT = 24 * 1024 * 1024
MESH = pl.DeviceIdType.MESH


def block_terms(running, col_blocks, index_block, tile_block, live_block):
    picked = col_blocks[index_block[:, 1]]
    kept = jnp.where(live_block[:, None, None], tile_block, jnp.zeros_like(tile_block))
    product = jnp.einsum("kij,kjf->kif", kept, picked, preferred_element_type=jnp.float32)
    flattened = product.reshape(product.shape[0], -1)
    return running.at[index_block[:, 0]].add(flattened)


def local_sparse(features, in_degree, tile_index, tile_count, adjacency_tiles, projection, out_bias):
    feat_width = features.shape[1]
    tile_size = adjacency_tiles.shape[1]
    slot_total = adjacency_tiles.shape[0]
    gathered = lax.all_gather(features, "row", axis=0, tiled=True)
    col_blocks = gathered.reshape(gathered.shape[0] // tile_size, tile_size, feat_width)
    row_blocks = features.shape[0] * lax.axis_size("col") // tile_size
    live_count = tile_count[0]
    zeroed = jnp.zeros((row_blocks, tile_size * feat_width), jnp.float32)

    def one_step(running, offset):
        index_block = lax.dynamic_slice_in_dim(tile_index, offset, BLK, 0)
        tile_block = lax.dynamic_slice_in_dim(adjacency_tiles, offset, BLK, 0)
        live_block = offset + jnp.arange(BLK, dtype=jnp.int32) < live_count
        return (block_terms(running, col_blocks, index_block, tile_block, live_block), None)

    summed, _ = lax.scan(one_step, zeroed, jnp.arange(0, slot_total, BLK, dtype=jnp.int32))
    partial_value = summed.reshape(row_blocks * tile_size, feat_width)
    own_sums = lax.psum_scatter(partial_value, "col", scatter_dimension=0, tiled=True)
    neighbour_mean = (own_sums / in_degree[:, None].astype(jnp.float32)).astype(jnp.bfloat16)
    joined = jnp.concatenate([features, neighbour_mean], axis=1)
    mixed = jnp.dot(joined, projection, preferred_element_type=jnp.float32) + out_bias[None, :]
    return jnp.maximum(mixed, 0.0).astype(jnp.bfloat16)


def densify_kernel(count_ref, place_ref, tiles_ref, dense_ref, stage, sems):
    slots, tile = stage.shape[0], stage.shape[1]
    per = slots // CHUNKS

    def load(i):
        part = pl.ds(i * per, per)
        return pltpu.make_async_copy(tiles_ref.at[part], stage.at[part], sems.at[i])

    for i in range(CHUNKS):
        load(i).start()

    @pl.loop(0, dense_ref.shape[0])
    def _(j):
        dense_ref[j] = jnp.zeros(dense_ref.shape[1:], dense_ref.dtype)

    count = count_ref[0]
    for i in range(CHUNKS):
        load(i).wait()

        @pl.loop(i * per, jnp.minimum((i + 1) * per, jnp.maximum(count, i * per)))
        def _(slot):
            col = place_ref[1, slot]
            row = pl.multiple_of(place_ref[0, slot] * tile, tile)
            dense_ref[col, pl.ds(row, tile), :] += stage[slot]


def fused_kernel(n_row, n_col, feat_ref, dense_ref, degree_ref, proj_ref, bias_ref, out_ref,
                 gathered, acc, hidden, degree_col, send, relayed, landed,
                 ag_send, ag_recv, send_sem, relay_sem, land_sem):
    seg, width = feat_ref.shape
    halves = width // LANES
    blocks = seg // LANES
    chips = n_row // 2
    r = lax.axis_index("row")
    c = lax.axis_index("col")
    sibling = r ^ 1

    barrier = pltpu.get_barrier_semaphore()

    def greet(row, col):
        pl.semaphore_signal(barrier, inc=1, device_id=(row, col), device_id_type=MESH)

    greet(sibling, c)
    for m in range(1, chips):
        greet(r ^ (2 * m), c)

    peers = chips
    for hop in range(1, n_col):
        for step in (-hop, hop):
            inside = (c + step >= 0) & (c + step < n_col)
            peers = peers + jnp.where(inside, 1, 0)

            @pl.when(inside)
            def _():
                greet(r, c + step)

    pl.semaphore_wait(barrier, peers)

    def lanes(h):
        return pl.ds(h * LANES, LANES)

    def gather_copy(h, j):
        if j == 0:
            src, owner, target = feat_ref.at[:, lanes(h)], r, sibling
        elif j < chips:
            src, owner, target = feat_ref.at[:, lanes(h)], r, r ^ (2 * j)
        else:
            owner = r ^ (2 * (j - chips + 1))
            src, target = gathered.at[owner, :, lanes(h)], sibling
        return pltpu.make_async_remote_copy(
            src_ref=src, dst_ref=gathered.at[owner, :, lanes(h)],
            send_sem=ag_send.at[h, j], recv_sem=ag_recv.at[h, j],
            device_id=(target, c), device_id_type=MESH)

    def source(j):
        if j == 0:
            return sibling
        if j < chips:
            return r ^ (2 * j)
        return sibling ^ (2 * (j - chips + 1))

    total = 2 * chips - 1

    def gather_start(h):
        for j in range(1, chips):
            gather_copy(h, j).start()
        gather_copy(h, 0).start()

    gather_start(0)

    def multiply(h, owner, block, first):
        @pl.loop(0, n_col)
        def _(d):
            rows = pl.ds(pl.multiple_of(d * seg, seg), seg)
            left = jnp.concatenate(
                [dense_ref[owner * blocks + k, rows, :] for k in range(blocks)], axis=1)
            product = jnp.dot(left, block, preferred_element_type=jnp.float32)
            if first:
                acc[h, rows, :] = product
            else:
                acc[h, rows, :] += product

    def own_block(h):
        multiply(h, r, feat_ref[:, lanes(h)], True)

    def other_block(h, j):
        gather_copy(h, j).wait_recv()
        if 0 < j < chips:
            gather_copy(h, j + chips - 1).start()
        owner = source(j)
        multiply(h, owner, gathered[owner, :, lanes(h)], False)

    def term(h, d):
        return acc[h, d * seg:(d + 1) * seg, :]

    def relay_copy(h, d, way):
        return pltpu.make_async_remote_copy(
            src_ref=send.at[h, d], dst_ref=relayed.at[h],
            send_sem=send_sem.at[h, d], recv_sem=relay_sem.at[h],
            device_id=(r, c + way), device_id_type=MESH)

    def land_copy(h, d, slot):
        return pltpu.make_async_remote_copy(
            src_ref=send.at[h, d], dst_ref=landed.at[h, slot],
            send_sem=send_sem.at[h, d], recv_sem=land_sem.at[h, slot],
            device_id=(r, d), device_id_type=MESH)

    def routes():
        for d in range(n_col - 1, -1, -1):
            for c_from in range(n_col):
                if c_from != d:
                    yield d, c_from, abs(d - c_from), 1 if d > c_from else -1

    def slot_of(hops, way):
        return hops - 1 + (0 if way > 0 else 2)

    def adds_relay(d, c_from, hops, way):
        return hops == 2 and 0 <= c_from - way < n_col

    def relays(c_from):
        return n_col == 4 and c_from in (0, n_col - 1)

    def send_direct(h, d, hops, way):
        send[h, d] = term(h, d).astype(send.dtype)
        land_copy(h, d, slot_of(hops, way)).start()

    def first_sends(h):
        for d, c_from, hops, way in routes():
            if hops == 3:
                @pl.when(c == c_from)
                def _():
                    send[h, d] = term(h, d).astype(send.dtype)
                    relay_copy(h, d, way).start()
            elif not relays(c_from) and not adds_relay(d, c_from, hops, way):
                @pl.when(c == c_from)
                def _():
                    send_direct(h, d, hops, way)

    def later_sends(h):
        for c_from in range(n_col):
            if relays(c_from):
                @pl.when(c == c_from)
                def _():
                    far = n_col - 1 - c_from
                    way = 1 if far > c_from else -1
                    relay_copy(h, far, way).wait_send()
                    for hops in (2, 1):
                        send_direct(h, c_from + way * hops, hops, way)

    def relay_sends(h):
        for d, c_from, hops, way in routes():
            if adds_relay(d, c_from, hops, way):
                @pl.when(c == c_from)
                def _():
                    relay_copy(h, d, way).wait_recv()
                    send[h, d] = (term(h, d) + relayed[h].astype(jnp.float32)).astype(send.dtype)
                    land_copy(h, d, slot_of(hops, way)).start()

    def finish(h):
        own = pl.ds(pl.multiple_of(c * seg, seg), seg)
        for hops in (1, 2):
            for way in (1, -1):
                origin = c - way * hops

                @pl.when((origin >= 0) & (origin < n_col))
                def _():
                    slot = slot_of(hops, way)
                    land_copy(h, 0, slot).wait_recv()
                    acc[h, own, :] += landed[h, slot].astype(jnp.float32)

        mean = (acc[h, own, :] / degree_col[...]).astype(jnp.bfloat16)
        hidden[...] += jnp.dot(
            mean, proj_ref[width + h * LANES:width + (h + 1) * LANES, :],
            preferred_element_type=jnp.float32)

    for h in range(halves):
        own_block(h)
        if h == 0:
            hidden[...] = jnp.dot(
                feat_ref[...], proj_ref[:width, :],
                preferred_element_type=jnp.float32) + bias_ref[...]
            for b in range(blocks):
                one = degree_ref[b:b + 1, :].astype(jnp.float32)
                degree_col[b * LANES:(b + 1) * LANES, :] = jnp.transpose(
                    jnp.broadcast_to(one, (LANES, LANES)))
        for j in range(total):
            if h > 0 and j == 1:
                later_sends(h - 1)
                relay_sends(h - 1)
            other_block(h, j)
            if j == chips - 1 and h + 1 < halves:
                gather_start(h + 1)
        first_sends(h)
        if h > 0:
            finish(h - 1)
    later_sends(halves - 1)
    relay_sends(halves - 1)
    finish(halves - 1)
    out_ref[...] = jnp.maximum(hidden[...], 0.0).astype(out_ref.dtype)

    for h in range(halves):
        for j in range(total):
            gather_copy(h, j).wait_send()
        for d, c_from, hops, way in routes():
            if hops < 3:
                @pl.when(c == c_from)
                def _():
                    land_copy(h, d, slot_of(hops, way)).wait_send()


def local_dense(n_row, n_col, features, in_degree, tile_index, tile_count, adjacency_tiles, projection, out_bias):
    seg, width = features.shape
    slots, tile, _ = adjacency_tiles.shape
    row_blocks = seg * n_col // tile
    col_blocks = seg * n_row // tile
    halves = width // LANES
    vmem = pl.BlockSpec(memory_space=pltpu.VMEM)
    smem = pl.BlockSpec(memory_space=pltpu.SMEM)
    dense = pl.pallas_call(
        densify_kernel,
        out_shape=pltpu.VMEM((col_blocks, row_blocks * tile, tile), jnp.bfloat16),
        in_specs=[smem, smem, pl.BlockSpec(memory_space=pl.ANY)],
        out_specs=vmem,
        scratch_shapes=[
            pltpu.VMEM((slots, tile, tile), jnp.bfloat16),
            pltpu.SemaphoreType.DMA((CHUNKS,)),
        ],
        compiler_params=pltpu.CompilerParams(vmem_limit_bytes=42 * 1024 * 1024),
    )(tile_count, tile_index.T, adjacency_tiles)
    carry_sem = pltpu.SemaphoreType.DMA((halves, 4))
    gather_sem = pltpu.SemaphoreType.DMA((halves, n_row))
    return pl.pallas_call(
        functools.partial(fused_kernel, n_row, n_col),
        out_shape=jax.ShapeDtypeStruct((seg, projection.shape[1]), jnp.bfloat16),
        in_specs=[vmem] * 5,
        out_specs=vmem,
        scratch_shapes=[
            pltpu.VMEM((n_row, seg, width), jnp.bfloat16),
            pltpu.VMEM((halves, n_col * seg, LANES), jnp.float32),
            pltpu.VMEM((seg, projection.shape[1]), jnp.float32),
            pltpu.VMEM((seg, LANES), jnp.float32),
            pltpu.VMEM((halves, n_col, seg, LANES), jnp.bfloat16),
            pltpu.VMEM((halves, seg, LANES), jnp.bfloat16),
            pltpu.VMEM((halves, 4, seg, LANES), jnp.bfloat16),
            gather_sem, gather_sem,
            carry_sem, pltpu.SemaphoreType.DMA((halves,)), carry_sem,
        ],
        compiler_params=pltpu.CompilerParams(
            collective_id=0, has_side_effects=True, vmem_limit_bytes=24 * 1024 * 1024),
    )(features, dense, in_degree.reshape(seg // LANES, LANES), projection, out_bias[None, :])


def solution(mesh):
    n_row, n_col = mesh.shape["row"], mesh.shape["col"]

    def local(features, in_degree, tile_index, tile_count, adjacency_tiles, projection, out_bias):
        seg, width = features.shape
        slots, tile, _ = adjacency_tiles.shape
        dense_bytes = 2 * seg * n_row * seg * n_col
        fits = (
            dense_bytes <= DENSE_LIMIT and slots <= 256 and slots % CHUNKS == 0
            and tile == LANES and seg % LANES == 0 and width % LANES == 0
            and n_row >= 4 and n_row & (n_row - 1) == 0 and 2 <= n_col <= 4)
        args = (features, in_degree, tile_index, tile_count, adjacency_tiles, projection, out_bias)
        return local_dense(n_row, n_col, *args) if fits else local_sparse(*args)

    return jax.shard_map(
        local,
        mesh=mesh,
        in_specs=(
            P(("row", "col"), None),
            P(("row", "col")),
            P(("row", "col"), None),
            P(("row", "col")),
            P(("row", "col"), None, None),
            P(),
            P(),
        ),
        out_specs=P(("row", "col"), None),
        check_vma=False,
    )
```
